32 devices in a mesh: ma: 4 (over y, x), freq: 8 (over z, core).
Axes of the slice: x: 2, y: 2, z: 4, core: 2. Of those that a mesh axis runs over, the one named last changes fastest.
Arguments:
- m_table: int32 [8], P('ma'), may hold values from 0 to 1023, as said below
- retained_modes: int32 [8], P('ma'), may hold values from 128 to 512, as said below
- cycle_ids: int32 [32], P('ma'), may hold values from 1 to 2047, as said below
- kl_coeffs: bfloat16 [8, 4, 512], P('ma', None, 'freq'), may hold values from -6 to 6
- kl_vectors: bfloat16 [8, 512, 32, 512], P('ma', 'freq'), may hold values from -0.375 to 0.375
- beam_matrix: bfloat16 [8, 32, 1024, 512], P('ma', 'freq'), may hold values from -0.00390625 to 0.00390625
Outputs:
- sky_maps: float32 [32, 2, 32, 2048], P('ma', None, 'freq')
The draws below stay inside these ranges and needn't reach their ends.
Inputs may be any that keep to these rules, and one draw needn't show every extreme that they name: `m_table`: all distinct; slots 2 q and 2 q + 1 hold two numbers that sum to 1023. `retained_modes`: some slot keeps all 512 modes. `cycle_ids`: all distinct.
All inputs are finite; a program needn't handle non-finite values.
Results may differ from the reference program's by a relative error of at most 0.01.
Values may be sent and summed in bfloat16 or wider, within the bound.
A program may use at most 64 MiB of HBM per device.

```python
import math
import jax
import jax.numpy as jnp
from jax import lax

MMAX = 1024
NPHI = 2048
L = 1024
K = 512
NKL = 512
CH = 32
NSIDE = 512
MM = 8
R = 32


def paired_slots(key):
    chosen = jax.random.permutation(jax.random.fold_in(key, 3), MMAX // 2)[:MM // 2]
    has_zero = jnp.any(chosen == 0)
    place = jax.random.randint(jax.random.fold_in(key, 4), (), 0, MM // 2)
    forced = jnp.where(jnp.arange(MM // 2) == place, 0, chosen)
    chosen = jnp.where(has_zero, chosen, forced)
    paired = jnp.stack([chosen, MMAX - 1 - chosen], axis=1)
    return paired.reshape(MM).astype(jnp.int32)


def draw_m_table(key, part):
    return paired_slots(key)


def draw_retained_modes(key, part):
    counts = jax.random.randint(jax.random.fold_in(key, 1), (MM,), NKL // 4, NKL + 1)
    fullest = jax.random.randint(jax.random.fold_in(key, 2), (), 0, MM)
    return jnp.where(jnp.arange(MM) == fullest, NKL, counts).astype(jnp.int32)


def draw_cycle_ids(key, part):
    return (jax.random.permutation(key, 4 * NSIDE - 1)[:R] + 1).astype(jnp.int32)


def draw_kl_coeffs(key, part):
    m_values = paired_slots(key).astype(jnp.float32)
    exponent = 2.0 * m_values / float(MMAX - 1) - 1.7
    slot_scale = jnp.exp(math.log(10.0) * exponent)
    value_key = jax.random.fold_in(key, 11)
    base = jnp.clip(jax.random.normal(value_key, (MM, 4, NKL), jnp.float32), -3.0, 3.0)
    values = jnp.clip(base * slot_scale[:, None, None], -6.0, 6.0)
    return values.astype(jnp.bfloat16)


def spiked(entries, own_key, source, target, shards_of, factor):
    owner, partner = [(jnp.arange(entries.shape[position]) // (entries.shape[position] // shards_of)).reshape([-1 if axis == position else 1 for axis in range(entries.ndim)]) for position in (source, target)]
    chosen = jax.random.permutation(own_key, shards_of)[partner]
    strong = (owner == chosen) | (owner == (partner + shards_of // 2) % shards_of)
    return jnp.where(strong, factor * entries, entries)


def shard_levels(own_key, shape, pieces, least, top_value):
    def one(position, shards_of):
        draws = jax.random.uniform(jax.random.fold_in(jax.random.fold_in(own_key, 6), position), (shards_of,), jnp.float32, least / len(pieces), top_value / len(pieces))
        return jnp.repeat(jnp.exp(draws), shape[position] // shards_of).reshape((-1,) + (1,) * (len(shape) - position - 1))

    level = one(*pieces[0])
    for cut in pieces[1:]:
        level = level * one(*cut)
    return level


def gaussian(key, shape, deviation, bound, pieces=(), held_as=jnp.bfloat16):
    array = jax.random.normal(key, shape, jnp.float32) * deviation
    if len(pieces) > 0:
        array = shard_levels(key, shape, pieces, -0.22, 0.18) * array
    return jnp.clip(array, min=-bound, max=bound).astype(held_as)


def heavy_noise(rng, dims, spread, bound, pieces, heavy, kind=jnp.bfloat16):
    result = spread * jax.random.normal(rng, dims, jnp.float32)
    if pieces:
        result = result * shard_levels(rng, dims, pieces, -0.22, 0.18)
    return jnp.clip(spiked(result, jax.random.fold_in(rng, 3), *heavy), -bound, bound).astype(kind)


def setup_inputs(seed: int = 0) -> dict:
    streams_of = jax.random.split(jax.random.key(seed), 7)
    return {
        "m_table": draw_m_table(jax.random.fold_in(streams_of[6], 71), 0),
        "retained_modes": draw_retained_modes(jax.random.fold_in(streams_of[6], 71), 0),
        "cycle_ids": draw_cycle_ids(jax.random.fold_in(streams_of[6], 71), 0),
        "kl_coeffs": draw_kl_coeffs(jax.random.fold_in(streams_of[6], 71), 0),
        "kl_vectors": heavy_noise(streams_of[4], (MM, NKL, CH, K), NKL ** -0.5, 0.375, ((0, 4), (1, 8)), (1, 2, 8, 2.0)),
        "beam_matrix": gaussian(streams_of[5], (MM, CH, L, K), (4 * K * L) ** -0.5, 0.00390625, ((0, 4), (1, 8))),
    }


def cycle_angles(cycle_numbers):
    cycle_float = cycle_numbers.astype(jnp.float32)
    nside_float = float(NSIDE)
    from_pole = jnp.minimum(cycle_float, 4.0 * nside_float - cycle_float)
    hemisphere = jnp.where(cycle_float <= 2.0 * nside_float, 1.0, -1.0)
    polar_part = from_pole * from_pole / (3.0 * nside_float * nside_float)
    colatitude_cosine = 1.0 - polar_part
    polar_sin = from_pole / (math.sqrt(3.0) * nside_float) * jnp.sqrt(2.0 - polar_part)
    latitude_cosine = 4.0 / 3.0 - 2.0 * from_pole / (3.0 * nside_float)
    latitude_sine = jnp.sqrt(jnp.maximum(1.0 - latitude_cosine * latitude_cosine, 0.25))
    in_cap = from_pole < nside_float
    cos_theta = hemisphere * jnp.where(in_cap, colatitude_cosine, latitude_cosine)
    sin_theta = jnp.where(in_cap, polar_sin, latitude_sine)
    return (cos_theta, sin_theta)

def combine(before_part, after_part):
    upper_left = after_part[0] * before_part[0] + after_part[1] * before_part[2]
    upper_right = after_part[0] * before_part[1] + after_part[1] * before_part[3]
    lower_left = after_part[2] * before_part[0] + after_part[3] * before_part[2]
    lower_right = after_part[2] * before_part[1] + after_part[3] * before_part[3]
    weight = jnp.abs(upper_left) + jnp.abs(upper_right) + jnp.abs(lower_left) + jnp.abs(lower_right)
    return (upper_left / weight, upper_right / weight, lower_left / weight, lower_right / weight, before_part[4] + after_part[4] + jnp.log(weight))

def legendre_rows(m_value, cos_theta, sin_theta):
    m_float = m_value.astype(jnp.float32)
    offset_rows = jnp.arange(L, dtype=jnp.float32)[:, None]
    later_rows = jnp.maximum(offset_rows, 2.0)
    degree = m_float + later_rows
    factor = jnp.sqrt((4.0 * degree * degree - 1.0) / (later_rows * (degree + m_float)))
    damping = jnp.sqrt((later_rows - 1.0) * (degree - 1.0 + m_float) / (4.0 * (degree - 1.0) * (degree - 1.0) - 1.0))
    first_step = jnp.sqrt(2.0 * m_float + 3.0)
    grid_shape = (L, cos_theta.shape[0])
    upper_left = jnp.where(offset_rows >= 2.0, factor * cos_theta[None, :], jnp.where(offset_rows >= 1.0, first_step * cos_theta[None, :], 1.0))
    upper_left = jnp.broadcast_to(upper_left, grid_shape)
    upper_right = jnp.broadcast_to(jnp.where(offset_rows >= 2.0, -factor * damping, 0.0), grid_shape)
    lower_left = jnp.broadcast_to(jnp.where(offset_rows >= 1.0, 1.0, 0.0), grid_shape)
    lower_right = jnp.broadcast_to(jnp.where(offset_rows >= 1.0, 0.0, 1.0), grid_shape)
    weight = jnp.abs(upper_left) + jnp.abs(upper_right) + jnp.abs(lower_left) + jnp.abs(lower_right)
    elements = (upper_left / weight, upper_right / weight, lower_left / weight, lower_right / weight, jnp.log(weight))
    prefix = lax.associative_scan(combine, elements, axis=0)
    log_start = 0.5 * (jnp.log((2.0 * m_float + 1.0) / (4.0 * math.pi)) + lax.lgamma(m_float + 0.5) - 0.5 * math.log(math.pi) - lax.lgamma(m_float + 1.0))
    log_start = log_start + m_float * jnp.log(sin_theta)[None, :]
    return prefix[0] * jnp.exp(prefix[4] + log_start)

def synthesize(harmonic_slot, m_value, cos_theta, sin_theta):
    channels = harmonic_slot.shape[0]
    flat_rows = harmonic_slot.reshape(channels * 4, L)
    padded = jnp.concatenate([flat_rows, jnp.zeros_like(flat_rows)], axis=1)
    shifted = lax.dynamic_slice_in_dim(padded, m_value.astype(jnp.int32), L, 1)
    legendre = legendre_rows(m_value, cos_theta, sin_theta).astype(jnp.bfloat16)
    synth_maps = jnp.dot(shifted, legendre, preferred_element_type=jnp.float32)
    return synth_maps.astype(jnp.bfloat16).reshape(channels, 2, 2, cos_theta.shape[0])

def fourier_table(m_values):
    azimuth_angle = jnp.arange(NPHI, dtype=jnp.int32)
    phase_index = m_values.astype(jnp.int32)[:, None] * azimuth_angle[None, :] % NPHI
    angle_table = phase_index.astype(jnp.float32) * (2.0 * math.pi / NPHI)
    weight = jnp.where(m_values == 0, 1.0, 2.0)[:, None]
    return jnp.stack([weight * jnp.cos(angle_table), -weight * jnp.sin(angle_table)]).astype(jnp.bfloat16)

def reference(m_table, retained_modes, cycle_ids, kl_coeffs, kl_vectors, beam_matrix):
    cos_theta, sin_theta = cycle_angles(cycle_ids)

    def per_slot(slot_entry):
        coeffs, vectors, beam_position, m_value, kept_count = slot_entry
        mode_index = jnp.arange(NKL, dtype=jnp.int32)
        masked = jnp.where(mode_index[None, :] < kept_count, coeffs, jnp.zeros_like(coeffs))
        svd_flat = jnp.dot(masked, vectors.reshape(NKL, CH * K), preferred_element_type=jnp.float32)
        singular_coefficients = svd_flat.astype(jnp.bfloat16).reshape(4, CH, K)
        spherical_harmonic = jnp.einsum('exd,xgd->xeg', singular_coefficients.astype(jnp.float32), beam_position.astype(jnp.float32)).astype(jnp.bfloat16)
        return synthesize(spherical_harmonic, m_value, cos_theta, sin_theta)
    cycle_modes = lax.map(per_slot, (kl_coeffs, kl_vectors, beam_matrix, m_table, retained_modes))
    fourier = fourier_table(m_table)
    return jnp.einsum('mcsqr,qmt->rsct', cycle_modes.astype(jnp.float32), fourier.astype(jnp.float32))
```

```python
import functools
import math

import jax
import jax.numpy as jnp
from jax import lax
from jax.experimental import pallas as pl
from jax.experimental.pallas import tpu as pltpu
from jax.sharding import PartitionSpec as P

NPHI = 2048
NSIDE = 512
STEPS = 32
LANES = 128
MESH = pl.DeviceIdType.MESH
F32 = jnp.float32
BF16 = jnp.bfloat16
BIG = 2.0**30
SHRINK = 2.0**-60


def cycle_angles(cycle_numbers):
    cycle_float = cycle_numbers.astype(F32)
    nside_float = float(NSIDE)
    from_pole = jnp.minimum(cycle_float, 4.0 * nside_float - cycle_float)
    hemisphere = jnp.where(cycle_float <= 2.0 * nside_float, 1.0, -1.0)
    polar_part = from_pole * from_pole / (3.0 * nside_float * nside_float)
    polar_sin = from_pole / (math.sqrt(3.0) * nside_float) * jnp.sqrt(2.0 - polar_part)
    latitude_cosine = 4.0 / 3.0 - 2.0 * from_pole / (3.0 * nside_float)
    latitude_sine = jnp.sqrt(jnp.maximum(1.0 - latitude_cosine * latitude_cosine, 0.25))
    in_cap = from_pole < nside_float
    cos_theta = hemisphere * jnp.where(in_cap, 1.0 - polar_part, latitude_cosine)
    sin_theta = jnp.where(in_cap, polar_sin, latitude_sine)
    return (cos_theta, sin_theta)


def central_ratio(m_float):
    shifted = m_float + 0.25
    inverse = 1.0 / (shifted * shifted)
    series = 1.0 + inverse * (-1.0 / 64.0 + inverse * (21.0 / 8192.0))
    ratio = series / jnp.sqrt(math.pi * shifted)
    exact = 1.0
    for m in range(8):
        ratio = jnp.where(m_float == float(m), exact, ratio)
        exact = exact * (2 * m + 1) / (2 * m + 2)
    return ratio


def start_values(m, sin_theta):
    mantissa = jnp.sqrt((2.0 * m + 1.0) * (1.0 / (4.0 * math.pi)) * central_ratio(m))
    power = m * (jnp.log(sin_theta) * (1.0 / math.log(2.0)))
    whole = jnp.floor(power)
    return (mantissa * jnp.exp2(power - whole), whole)


def turn_cosine(turns):
    half = NPHI // 2
    u = NPHI // 4 - jnp.abs((turns & (NPHI - 1)) - half)
    x = u.astype(F32) * (2.0 * math.pi / NPHI)
    z = x * x
    series = -1.0 / 39916800.0
    for coefficient in (1.0 / 362880.0, -1.0 / 5040.0, 1.0 / 120.0, -1.0 / 6.0, 1.0):
        series = coefficient + z * series
    return -x * series


def rescaled(values, exponent):
    size = functools.reduce(jnp.maximum, [jnp.abs(v) for v in values])
    large, small = size > BIG, size < 1.0 / BIG
    scale = jnp.where(large, SHRINK, jnp.where(small, 1.0 / SHRINK, 1.0))
    shift = jnp.where(large, 60.0, jnp.where(small, -60.0, 0.0))
    return [v * scale for v in values], exponent + shift


def product(after, before, exponent):
    a, b, c, d = after
    p, q, r, s = before
    return rescaled([a * p + b * r, a * q + b * s, c * p + d * r, c * q + d * s], exponent)


def legendre_into(m_values, cos_theta, sin_theta, cycles, length, u_ref, v_ref, leg_ref):
    slots = len(m_values)
    parts = LANES // cycles
    blocks = length // (STEPS * 8 * parts)
    assert blocks == 1 or parts == 1
    shape = (8, LANES)
    sub = lax.broadcasted_iota(jnp.int32, shape, 0)
    part = lax.broadcasted_iota(jnp.int32, shape, 1) // cycles
    c = jnp.broadcast_to(cos_theta, shape)
    bases = [
        (((b * parts + part) * 8 + sub) * STEPS).astype(F32)
        for _ in range(slots) for b in range(blocks)
    ]
    ms = [m_values[s] for s in range(slots) for _ in range(blocks)]

    def ratio(degree, m):
        after = degree - m > 0.5
        y = (degree - m) * (degree + m) / ((2.0 * degree - 1.0) * (2.0 * degree + 1.0))
        y = jnp.where(after, y, 1.0)
        a = lax.rsqrt(y)
        a = a * (1.5 - 0.5 * y * a * a)
        return (after, a, jnp.where(after, y * a, 0.0))

    unroll = 8

    def body(i, state):
        for k in range(unroll):
            t = i * unroll + k
            later = []
            for j, (u1, u2, v1, v2, root) in enumerate(state):
                after, a, next_root = ratio(bases[j] + t.astype(F32), ms[j])
                alpha = jnp.where(after, a * c, 1.0)
                beta = a * root
                u = alpha * u1 - beta * u2
                v = alpha * v1 - beta * v2
                u_ref[j, t] = u
                v_ref[j, t] = v
                later.append((u, u1, v, v1, next_root))
            state = tuple(later)
        return state

    one, zero = jnp.ones(shape, F32), jnp.zeros(shape, F32)
    state = tuple(
        (one, zero, zero, one, ratio(base - 1.0, m)[2]) for base, m in zip(bases, ms)
    )
    state = lax.fori_loop(0, STEPS // unroll, body, state)
    log_starts = [start_values(jnp.full((1, LANES), m, F32), sin_theta) for m in m_values]
    for j, (u1, u2, v1, v2, _) in enumerate(state):
        s, b = j // blocks, j % blocks
        matrix, exponent = rescaled([u1, v1, u2, v2], zero)
        matrix, exponent = rescaled(matrix, exponent)
        for d in (1, 2, 4):
            low = sub < d
            before = [
                jnp.where(low, unit, pltpu.roll(x, d, 0))
                for x, unit in zip(matrix, (1.0, 0.0, 0.0, 1.0))
            ]
            carried = jnp.where(low, 0.0, pltpu.roll(exponent, d, 0))
            matrix, exponent = product(matrix, before, exponent + carried)
        if b == 0:
            x, e = (jnp.broadcast_to(v, shape) for v in log_starts[s])
            y = zero
        whole = [jnp.broadcast_to(v[7:8], shape) for v in matrix]
        whole_e = jnp.broadcast_to(exponent[7:8], shape)
        for k in range(parts - 1, 0, -1):
            here = part >= k
            t00, t01, t10, t11, te = (pltpu.roll(v, k * cycles, 1) for v in whole + [whole_e])
            (x2, y2), e2 = rescaled([t00 * x + t01 * y, t10 * x + t11 * y], e + te)
            x, y, e = jnp.where(here, x2, x), jnp.where(here, y2, y), jnp.where(here, e2, e)
        low = sub < 1
        s00, s01, s10, s11 = (
            jnp.where(low, unit, pltpu.roll(v, 1, 0))
            for v, unit in zip(matrix, (1.0, 0.0, 0.0, 1.0))
        )
        total_e = e + jnp.where(low, 0.0, pltpu.roll(exponent, 1, 0))
        half = jnp.floor(total_e * 0.5)
        scale = jnp.exp2(jnp.clip(half, -126.0, 126.0))
        first = jnp.exp2(jnp.clip(total_e - half, -126.0, 126.0))
        start_x = (s00 * x + s01 * y) * first
        start_y = (s10 * x + s11 * y) * first
        for t in range(STEPS):
            value = (u_ref[j, t] * start_x + v_ref[j, t] * start_y) * scale
            u_ref[j, t] = jnp.where(bases[j] + float(t) >= ms[j], value, 0.0)
        if b < blocks - 1:
            t00, t01, t10, t11 = whole
            (x, y), e = rescaled([t00 * x + t01 * y, t10 * x + t11 * y], e + whole_e)
        stack = LANES // STEPS
        for a in range(8 // stack):
            tall = jnp.concatenate(
                [u_ref[j, :, a * stack + k, :] for k in range(stack)], axis=0
            )
            turned = tall.T
            for g in range(parts):
                at = ((b * parts + g) * 8 + a * stack) * STEPS
                leg_ref[s * cycles : (s + 1) * cycles, at : at + LANES] = turned[
                    g * cycles : (g + 1) * cycles
                ].astype(BF16)


def main_kernel(
    n_ma, n_freq, m_hbm, kept_hbm, cyc_hbm, coef_hbm, vec_hbm, beam_hbm, sum_out, table_out,
    m_ref, kept_ref, cyc_ref, coef, vec, beam, ints, ints_send, part, precv, zsend, zrecv,
    u_ref, v_ref, leg, tab, svd, modes, mrecv,
    small_sem, vec_sem, beam_sem, isend_sem, irecv_sem, dsend_sem, drecv_sem,
    zsend_sem, zrecv_sem, msend_sem, mrecv_sem,
):
    slots, quads, n_modes = coef.shape
    n_groups, _, _, span, depth = vec.shape
    channels, length = beam.shape[1:3]
    n_cyc = cyc_hbm.shape[0]
    cycles = n_cyc * n_ma
    n_z = n_freq // 2
    per_group = n_z // n_groups
    rows = channels * quads
    wide = svd.shape[0]
    ma, fr = lax.axis_index("ma"), lax.axis_index("freq")
    z, core = fr // 2, lax.rem(fr, 2)
    other = 1 - core
    partner = z * 2 + other
    my_group, my_place = z // per_group, lax.rem(z, per_group)

    def reached(x):
        return (x + n_groups) // n_groups

    upper = reached(2 * my_group - n_groups)

    def group_at(o):
        if o == n_groups - 1:
            return my_group
        low = n_groups - 1 - o
        return upper * (o + reached(o - my_group)) + (1 - upper) * (low - reached(my_group - low))

    smalls = [
        pltpu.make_async_copy(src, dst, small_sem.at[i])
        for i, (src, dst) in enumerate(
            [(coef_hbm, coef), (kept_hbm, kept_ref), (m_hbm, m_ref), (cyc_hbm, cyc_ref)]
        )
    ]
    for copy in smalls:
        copy.start()
    vec_copies = [
        [
            pltpu.make_async_copy(
                vec_hbm.at[s, :, pl.ds(pl.multiple_of(group_at(o) * span, span), span), :],
                vec.at[o, s], vec_sem.at[o, s],
            )
            for s in range(slots)
        ]
        for o in range(n_groups)
    ]
    beam_copies = [
        [
            pltpu.make_async_copy(beam_hbm.at[s, c], beam.at[s, c], beam_sem.at[s, c])
            for c in range(channels)
        ]
        for s in range(slots)
    ]
    for pair in vec_copies:
        for copy in pair:
            copy.start()

    barrier = pltpu.get_barrier_semaphore()
    for k in range(1, n_ma):
        pl.semaphore_signal(
            barrier, inc=1, device_id=(lax.rem(ma + k, n_ma), fr), device_id_type=MESH
        )
    for k in range(1, n_z):
        pl.semaphore_signal(
            barrier, inc=1, device_id=(ma, lax.rem(fr + 2 * k, n_freq)), device_id_type=MESH
        )
    pl.semaphore_signal(barrier, inc=1, device_id=(ma, partner), device_id_type=MESH)

    svd[...] = jnp.zeros_like(svd)
    flat_wide = n_modes * span
    row = lax.broadcasted_iota(jnp.int32, (span * quads, flat_wide), 0)
    column = lax.broadcasted_iota(jnp.int32, (span * quads, flat_wide), 1)
    same_channel = row // quads == column % span
    spread = (
        lax.broadcasted_iota(jnp.int32, (n_modes, flat_wide), 1) // span
        == lax.broadcasted_iota(jnp.int32, (n_modes, flat_wide), 0)
    )
    spread = jnp.where(spread, 1.0, 0.0).astype(BF16)
    mode = fr * n_modes + lax.broadcasted_iota(jnp.int32, (quads, n_modes), 1)
    smalls[0].wait()
    smalls[1].wait()
    weights = []
    for s in range(slots):
        masked = jnp.where(mode < kept_ref[s], coef[s].astype(F32), 0.0)
        tall = jnp.concatenate([masked] * span, axis=0).astype(BF16)
        full = jnp.dot(tall, spread, preferred_element_type=F32)
        weights.append(jnp.where(same_channel, full, 0.0).astype(BF16))
    smalls[2].wait()
    smalls[3].wait()
    lane = lax.broadcasted_iota(jnp.int32, (8, LANES), 1)
    line = lax.broadcasted_iota(jnp.int32, (8, LANES), 0)
    packed = jnp.zeros((8, LANES), jnp.int32)
    for i in range(n_cyc):
        here = (line == 0) & (lane % cycles == ma * n_cyc + i)
        packed = jnp.where(here, cyc_ref[i], packed)
    for s in range(slots):
        packed = jnp.where((line == 1) & (lane == ma * slots + s), m_ref[s], packed)
    ints_send[...] = packed

    int_copies, pair_copies = [], []
    for o in range(n_groups):
        for s in range(slots):
            vec_copies[o][s].wait()
            flat = vec[o, s].reshape(flat_wide, depth)
            value = jnp.dot(weights[s], flat, preferred_element_type=F32).astype(BF16)
            for j in range(per_group):
                for k in range(2):
                    at = (j * 2 + k) * rows
                    part[o, k, j, s] = value[at : at + rows]
        if o == 0:
            pl.semaphore_wait(barrier, n_ma - 1 + n_z - 1 + 1)
        copy = pltpu.make_async_remote_copy(
            src_ref=part.at[o, other], dst_ref=precv.at[o], send_sem=dsend_sem.at[o],
            recv_sem=drecv_sem.at[o], device_id=(ma, partner), device_id_type=MESH,
        )
        copy.start()
        pair_copies.append(copy)
        if o == 0:
            for k in range(1, n_ma):
                copy = pltpu.make_async_remote_copy(
                    src_ref=ints_send, dst_ref=ints.at[k], send_sem=isend_sem.at[k],
                    recv_sem=irecv_sem.at[k], device_id=(lax.rem(ma + k, n_ma), fr),
                    device_id_type=MESH,
                )
                copy.start()
                int_copies.append(copy)
            for group in beam_copies:
                for copy in group:
                    copy.start()

    z_copies = []
    for o in range(n_groups):
        pair_copies[o].wait_recv()
        joined = part[o, core].astype(F32) + precv[o].astype(F32)
        zsend[o] = joined.astype(BF16)
        for step in range(1 if o == n_groups - 1 else 0, per_group):
            j = lax.rem(my_place + step, per_group)
            to = group_at(o) * per_group + j
            k = lax.rem(to - z + n_z, n_z)
            copy = pltpu.make_async_remote_copy(
                src_ref=zsend.at[o, j], dst_ref=zrecv.at[k],
                send_sem=zsend_sem.at[o, step], recv_sem=zrecv_sem.at[k],
                device_id=(ma, to * 2 + core), device_id_type=MESH,
            )
            copy.start()
            z_copies.append(copy)

    for copy in int_copies:
        copy.wait_recv()
    for k in range(1, n_ma):
        packed = packed + ints[k]
    cos_theta, sin_theta = cycle_angles(packed[0:1])
    m_values = [m_ref[s].astype(F32) for s in range(slots)]
    legendre_into(m_values, cos_theta, sin_theta, cycles, length, u_ref, v_ref, leg)
    for s in range(slots):
        for c in range(channels):
            beam_copies[s][c].wait()
            value = jnp.dot(
                leg[s * cycles : (s + 1) * cycles, :], beam[s, c], preferred_element_type=F32
            )
            at = (s * channels + c) * cycles
            tab[at : at + cycles] = value.astype(BF16)

    n_lines = n_ma * slots * 2
    line = lax.broadcasted_iota(jnp.int32, (n_lines, LANES), 0)
    lane = lax.broadcasted_iota(jnp.int32, (n_lines, LANES), 1)
    m_all = jnp.broadcast_to(packed[1:2].astype(F32), (n_lines, LANES))
    m_column = jnp.sum(jnp.where(lane == line // 2, m_all, 0.0), axis=1, keepdims=True)
    line = lax.broadcasted_iota(jnp.int32, (n_lines, NPHI), 0)
    time = lax.broadcasted_iota(jnp.int32, (n_lines, NPHI), 1)
    m = jnp.broadcast_to(m_column.astype(jnp.int32), (n_lines, NPHI))
    table = turn_cosine(m * time + (line % 2) * (NPHI // 4))
    table = (jnp.where(m == 0, 1.0, 2.0) * table).astype(BF16)
    to_row = lax.broadcasted_iota(jnp.int32, (wide, n_lines), 0)
    from_row = lax.broadcasted_iota(jnp.int32, (wide, n_lines), 1)
    pick = to_row // (quads * channels) * 2 + to_row % 2 == from_row
    pick = jnp.where(pick, 1.0, 0.0).astype(BF16)
    table_out[...] = jnp.dot(pick, table, preferred_element_type=F32).astype(BF16)

    total = zsend[n_groups - 1, my_place].astype(F32)
    for k in range(1, n_z):
        pltpu.make_async_remote_copy(
            src_ref=zsend.at[0, 0], dst_ref=zrecv.at[k], send_sem=zsend_sem.at[0, 0],
            recv_sem=zrecv_sem.at[k], device_id=(ma, fr), device_id_type=MESH,
        ).wait_recv()
        total = total + zrecv[k].astype(F32)
    mine = slots * rows
    svd[pl.ds(pl.multiple_of(ma * mine, mine), mine), :] = total.reshape(mine, depth).astype(BF16)
    every = lax.dot_general(
        tab[...], svd[...], (((1,), (1,)), ((), ())), preferred_element_type=F32
    )
    lane = lax.broadcasted_iota(jnp.int32, (cycles, wide), 1)
    owner = lane // quads % (slots * channels)
    chosen = jnp.zeros((cycles, wide), F32)
    for i in range(slots * channels):
        chosen = jnp.where(owner == i, every[i * cycles : (i + 1) * cycles], chosen)
    modes[...] = chosen.reshape(n_ma, n_cyc, wide)
    mode_copies = []
    for k in range(1, n_ma):
        to = lax.rem(ma + k, n_ma)
        copy = pltpu.make_async_remote_copy(
            src_ref=modes.at[to], dst_ref=mrecv.at[k], send_sem=msend_sem.at[k],
            recv_sem=mrecv_sem.at[k], device_id=(to, fr), device_id_type=MESH,
        )
        copy.start()
        mode_copies.append(copy)
    for copy in int_copies + pair_copies + z_copies:
        copy.wait_send()
    gathered = modes[ma]
    for copy in mode_copies:
        copy.wait_recv()
    for k in range(1, n_ma):
        gathered = gathered + mrecv[k]
    sum_out[...] = gathered
    for copy in mode_copies:
        copy.wait_send()


def main_call(n_ma, n_freq, m_table, retained_modes, cycle_ids, kl_coeffs, kl_vectors, beam):
    slots, quads, n_modes = kl_coeffs.shape
    all_channels, depth = kl_vectors.shape[2:]
    channels, length = beam.shape[1:3]
    n_cyc = cycle_ids.shape[0]
    cycles = n_cyc * n_ma
    n_z = n_freq // 2
    span = max(8, 2 * channels)
    n_groups = all_channels // span
    per_group = n_z // n_groups
    rows = channels * quads
    wide = max(LANES, n_ma * slots * rows)
    blocks = slots * length // (STEPS * 8 * (LANES // cycles))
    held = (m_table, retained_modes, cycle_ids, kl_coeffs, kl_vectors, beam)
    hbm = pl.BlockSpec(memory_space=pltpu.HBM)
    vmem = pl.BlockSpec(memory_space=pltpu.VMEM)
    dma = pltpu.SemaphoreType.DMA
    return pl.pallas_call(
        functools.partial(main_kernel, n_ma, n_freq),
        out_shape=(
            jax.ShapeDtypeStruct((n_cyc, wide), F32),
            jax.ShapeDtypeStruct((wide, NPHI), BF16),
        ),
        in_specs=[hbm] * 6,
        out_specs=(vmem, vmem),
        scratch_shapes=[
            pltpu.SMEM((slots,), jnp.int32),
            pltpu.SMEM((slots,), jnp.int32),
            pltpu.SMEM((n_cyc,), jnp.int32),
            pltpu.VMEM(kl_coeffs.shape, BF16),
            pltpu.VMEM((n_groups, slots, n_modes, span, depth), BF16),
            pltpu.VMEM(beam.shape, BF16),
            pltpu.VMEM((n_ma, 8, LANES), jnp.int32),
            pltpu.VMEM((8, LANES), jnp.int32),
            pltpu.VMEM((n_groups, 2, per_group, slots, rows, depth), BF16),
            pltpu.VMEM((n_groups, per_group, slots, rows, depth), BF16),
            pltpu.VMEM((n_groups, per_group, slots, rows, depth), BF16),
            pltpu.VMEM((n_z, slots, rows, depth), BF16),
            pltpu.VMEM((blocks, STEPS, 8, LANES), F32),
            pltpu.VMEM((blocks, STEPS, 8, LANES), F32),
            pltpu.VMEM((slots * cycles, length), BF16),
            pltpu.VMEM((slots * channels * cycles, depth), BF16),
            pltpu.VMEM((wide, depth), BF16),
            pltpu.VMEM((n_ma, n_cyc, wide), F32),
            pltpu.VMEM((n_ma, n_cyc, wide), F32),
            dma((4,)),
            dma((n_groups, slots)),
            dma((slots, channels)),
            dma((n_ma,)),
            dma((n_ma,)),
            dma((n_groups,)),
            dma((n_groups,)),
            dma((n_groups, per_group)),
            dma((n_z,)),
            dma((n_ma,)),
            dma((n_ma,)),
        ],
        compiler_params=pltpu.CompilerParams(
            collective_id=0, has_side_effects=True, vmem_limit_bytes=32 * 2**20
        ),
        name="cycle_modes",
    )(*[pltpu.with_memory_space_constraint(x, pltpu.HBM) for x in held])


def sky_kernel(channels, sum_ref, table_ref, out_hbm, out, sem):
    n_cyc, wide = sum_ref.shape
    pieces, step = out.shape[0], out.shape[4]
    rows = n_cyc * 2 * channels
    row = lax.broadcasted_iota(jnp.int32, (rows, wide), 0)
    lane = lax.broadcasted_iota(jnp.int32, (rows, wide), 1)
    wanted = (lane // 4 % channels == row % channels) & (lane % 4 // 2 == row // channels % 2)
    spread = jnp.broadcast_to(sum_ref[...][:, None, :], (n_cyc, 2 * channels, wide))
    left = jnp.where(wanted, spread.reshape(rows, wide), 0.0).astype(BF16)
    copies = []
    for i in range(pieces):
        value = jnp.dot(
            left, table_ref[:, i * step : (i + 1) * step], preferred_element_type=F32
        )
        for r in range(n_cyc * 2):
            out[i, r // 2, r % 2] = value[r * channels : (r + 1) * channels]
        copy = pltpu.make_async_copy(
            out.at[i], out_hbm.at[:, :, :, pl.ds(i * step, step)], sem.at[i]
        )
        copy.start()
        copies.append(copy)
    for copy in copies:
        copy.wait()


def sky_call(channels, gathered, table):
    n_cyc = gathered.shape[0]
    pieces = 4
    return pl.pallas_call(
        functools.partial(sky_kernel, channels),
        out_shape=jax.ShapeDtypeStruct((n_cyc, 2, channels, NPHI), F32),
        in_specs=[pl.BlockSpec(memory_space=pltpu.VMEM)] * 2,
        out_specs=pl.BlockSpec(memory_space=pltpu.HBM),
        scratch_shapes=[
            pltpu.VMEM((pieces, n_cyc, 2, channels, NPHI // pieces), F32),
            pltpu.SemaphoreType.DMA((pieces,)),
        ],
        compiler_params=pltpu.CompilerParams(vmem_limit_bytes=16 * 2**20),
        name="sky_maps",
    )(gathered, table)


def local(n_ma, n_freq, m_table, retained_modes, cycle_ids, kl_coeffs, kl_vectors, beam_matrix):
    gathered, table = main_call(
        n_ma, n_freq, m_table, retained_modes, cycle_ids, kl_coeffs, kl_vectors, beam_matrix
    )
    return sky_call(beam_matrix.shape[1], gathered, table)


def solution(mesh):
    placed = (
        P("ma"),
        P("ma"),
        P("ma"),
        P("ma", None, "freq"),
        P("ma", "freq", None, None),
        P("ma", "freq", None, None),
    )
    return jax.shard_map(
        functools.partial(local, mesh.shape["ma"], mesh.shape["freq"]),
        mesh=mesh, in_specs=placed, out_specs=P("ma", None, "freq", None), check_vma=False,
    )
```
